32 devices in a mesh: gz: 16 (over z, y, core), ba: 2 (over x).
Axes of the slice: x: 2, y: 2, z: 4, core: 2. Of those that a mesh axis runs over, the one named last changes fastest.
Arguments:
- coeffs: float32 [2, 3, 4, 32, 128, 128], P(None, None, 'ba', 'gz'), may hold values from -6 to 6
- material: int32 [32, 128, 128], P('gz'), may hold values from 0 to 3
- inv_diag: float32 [4, 3], replicated, may hold values from 0.1 to 1
- inv_off: float32 [4, 3], replicated, may hold values from -0.1 to 0.1
Outputs:
- theta: float32 [2, 3, 4, 32, 128, 128], P(None, None, 'ba', 'gz')
- gram: float32 [2, 4, 4], P(None, None, 'ba')
The draws below stay inside these ranges and needn't reach their ends.
Inputs may be any that keep to these rules, and one draw needn't show every extreme that they name: material indices.
All inputs are finite; a program needn't handle non-finite values.
Results may differ from the reference program's by a relative error of at most 0.00011.
Values sent between devices are 32-bit elements; how exact they have to be, the bound alone decides.
A program may use at most 64 MiB of HBM per device.

```python
import math
import jax
import jax.numpy as jnp
from jax import lax

NX = 128
NY = 128
CZ = 2
MATERIALS = 4
NZ = 32
BANDS = 4
N_GZ = 16


def with_ends(values, stream_key, low, largest):
    index_at = [jax.random.randint(jax.random.fold_in(stream_key, axis), (), 0, length) for axis, length in enumerate(values.shape)]
    widest = values.shape.index(max(values.shape))
    next_to = index_at[:widest] + [(index_at[widest] + 1) % values.shape[widest]] + index_at[widest + 1:]
    return values.at[tuple(index_at)].set(low).at[tuple(next_to)].set(largest)


def block_levels(rng, extent, cuts, low, largest):
    def one(axis_at, blocks):
        heights = jax.random.uniform(jax.random.fold_in(jax.random.fold_in(rng, 6), axis_at), (blocks,), jnp.float32, low / len(cuts), largest / len(cuts))
        return jnp.repeat(jnp.exp(heights), extent[axis_at] // blocks).reshape((-1,) + (1,) * (len(extent) - axis_at - 1))

    factor_of = one(*cuts[0])
    for cut in cuts[1:]:
        factor_of = factor_of * one(*cut)
    return factor_of


def noise(key, extent, width, reach, cuts=(), kind=jnp.bfloat16):
    entries = jax.random.normal(key, extent, jnp.float32) * width
    if len(cuts) > 0:
        entries = block_levels(key, extent, cuts, -0.22, 0.18) * entries
    return jnp.clip(entries, min=-reach, max=reach).astype(kind)


def setup_inputs(seed: int = 0) -> dict:
    streams_of = jax.random.split(jax.random.key(seed), 5)
    return {
        "coeffs": noise(streams_of[0], (2, 3, BANDS, NZ, NY, NX), 1.0, 6.0, ((2, 2), (3, 16)), jnp.float32),
        "material": with_ends(jax.random.randint(streams_of[1], (NZ, NY, NX), 0, MATERIALS), jax.random.fold_in(streams_of[1], 1), 0, MATERIALS - 1).astype(jnp.int32),
        "inv_diag": jnp.clip(jnp.exp(jax.random.uniform(streams_of[2], (MATERIALS, 3), jnp.float32, math.log(0.1), math.log(1.0))), 0.1, 1.0),
        "inv_off": jnp.clip(jax.random.uniform(streams_of[3], (MATERIALS, 3), jnp.float32, -0.1, 0.1), -0.1, 0.1),
    }


highest = lax.Precision.HIGHEST


def reverse_bits(values, levels):
    flipped = jnp.zeros_like(values)
    for position in range(levels):
        flipped = flipped + ((values >> position) & 1) * (1 << (levels - 1 - position))
    return flipped


def signed_wave(numbers, length):
    shifted = jnp.where(numbers < length // 2, numbers, numbers - length)
    return shifted.astype(jnp.float32) / (length / 2.0)


def cross_waves(waves, field):
    first, second, third = waves
    return jnp.stack([second * field[2] - third * field[1],
                      third * field[0] - first * field[2],
                      first * field[1] - second * field[0]])


def reference(coeffs, material, inv_diag, inv_off):
    levels = N_GZ.bit_length() - 1
    rows = jnp.arange(NZ, dtype=jnp.int32)
    wave_rows = reverse_bits(rows // CZ, levels) + N_GZ * (rows % CZ)
    natural = jnp.zeros((NZ,), jnp.int32).at[wave_rows].set(rows)
    waves = (signed_wave(jnp.arange(NX, dtype=jnp.int32), NX)[None, None, :],
             signed_wave(jnp.arange(NY, dtype=jnp.int32), NY)[None, :, None],
             signed_wave(wave_rows, NZ)[:, None, None])
    onehot = (material[None] == jnp.arange(MATERIALS, dtype=jnp.int32)[:, None, None, None]).astype(jnp.float32)
    table = jnp.concatenate([inv_diag, inv_off], axis=1)
    tensor = jnp.einsum("mk,mzyx->kzyx", table, onehot, precision=highest)

    def one_band(band):
        spectral = band[0] + 1j * band[1]
        curl = cross_waves(waves, spectral)[:, natural]
        field = jnp.fft.ifftn(curl, axes=(1, 2, 3), norm="ortho")
        scaled = jnp.stack([tensor[0] * field[0] + tensor[3] * field[1] + tensor[5] * field[2],
                            tensor[3] * field[0] + tensor[1] * field[1] + tensor[4] * field[2],
                            tensor[5] * field[0] + tensor[4] * field[1] + tensor[2] * field[2]])
        back = jnp.fft.fftn(scaled, axes=(1, 2, 3), norm="ortho")[:, wave_rows]
        result = -cross_waves(waves, back)
        return jnp.stack([jnp.real(result), jnp.imag(result)]).astype(jnp.float32)

    theta = jnp.moveaxis(lax.map(one_band, jnp.moveaxis(coeffs, 2, 0)), 0, 2)
    factor = 1.0 / (NX * NY * NZ)
    real_part = (jnp.einsum("cbzyx,cezyx->be", coeffs[0], theta[0], precision=highest)
                 + jnp.einsum("cbzyx,cezyx->be", coeffs[1], theta[1], precision=highest)) * factor
    imag_part = (jnp.einsum("cbzyx,cezyx->be", coeffs[0], theta[1], precision=highest)
                 - jnp.einsum("cbzyx,cezyx->be", coeffs[1], theta[0], precision=highest)) * factor
    gram = jnp.stack([real_part, imag_part])
    return theta, gram
```

```python
import functools
import math

import jax
import jax.numpy as jnp
import numpy as np
from jax import lax
from jax.experimental import pallas as pl
from jax.experimental.pallas import tpu as pltpu
from jax.sharding import PartitionSpec as P

highest = lax.Precision.HIGHEST
half_turn = 3.141592653589793


def reverse_bits(values, levels):
    flipped = jnp.zeros_like(values)
    for position in range(levels):
        flipped = flipped + (values >> position & 1) * (1 << levels - 1 - position)
    return flipped


def signed_wave(numbers, length):
    shifted = jnp.where(numbers < length // 2, numbers, numbers - length)
    return shifted.astype(jnp.float32) / (length / 2.0)


def phase_tables(first, second, length, sign):
    product = first[:, None] * second[None, :] % length
    angle = 2.0 * half_turn / length * product.astype(jnp.float32)
    factor = 1.0 / math.sqrt(length)
    return (jnp.cos(angle) * factor, sign * jnp.sin(angle) * factor)


def cross_waves(waves, field):
    first, second, third = waves
    return jnp.stack(
        [
            second * field[:, 2] - third * field[:, 1],
            third * field[:, 0] - first * field[:, 2],
            first * field[:, 1] - second * field[:, 0],
        ],
        axis=1,
    )


def along_width(field, cosine, sine):
    breadth = field.shape[-1]
    rows = field.reshape(2, -1, breadth)
    joined = jnp.concatenate([cosine, sine], axis=1)
    real_prod = jnp.dot(rows[0], joined, precision=highest)
    imag_prod = jnp.dot(rows[1], joined, precision=highest)
    real_out = real_prod[:, :breadth] - imag_prod[:, breadth:]
    imag_out = real_prod[:, breadth:] + imag_prod[:, :breadth]
    return jnp.stack([real_out, imag_out]).reshape(field.shape)


def along_height(field, cosine, sine):
    tables = jnp.stack([cosine, sine])
    product = jnp.einsum("pcbzyx,tyk->tpcbzkx", field, tables, precision=highest)
    return jnp.stack([product[0, 0] - product[1, 1], product[1, 0] + product[0, 1]])


def along_depth(field, cosine, sine):
    tables = jnp.stack([cosine, sine])
    product = jnp.einsum("pcbzyx,tzk->tpcbkyx", field, tables, precision=highest)
    return jnp.stack([product[0, 0] - product[1, 1], product[1, 0] + product[0, 1]])


def apply_material(field, material, inv_diag, inv_off):
    materials = inv_diag.shape[0]
    onehot = (material[None] == jnp.arange(materials, dtype=jnp.int32)[:, None, None, None]).astype(
        jnp.float32
    )
    table = jnp.concatenate([inv_diag, inv_off], axis=1)
    tensor = jnp.einsum("mk,mzyx->kzyx", table, onehot, precision=highest)
    first = field[:, 0]
    second = field[:, 1]
    third = field[:, 2]
    return jnp.stack(
        [
            tensor[0] * first + tensor[3] * second + tensor[5] * third,
            tensor[3] * first + tensor[1] * second + tensor[4] * third,
            tensor[5] * first + tensor[4] * second + tensor[2] * third,
        ],
        axis=1,
    )


def on_device(coeffs, material, inv_diag, inv_off):
    groups = lax.axis_size("gz")
    levels = groups.bit_length() - 1
    depth = coeffs.shape[3]
    height = coeffs.shape[4]
    breadth = coeffs.shape[5]
    total_depth = depth * groups
    device = lax.axis_index("gz")
    local_rows = jnp.arange(depth, dtype=jnp.int32)
    waves_here = reverse_bits(device, levels) + groups * local_rows
    across = jnp.arange(breadth, dtype=jnp.int32)
    upward = jnp.arange(height, dtype=jnp.int32)
    waves = (
        signed_wave(across, breadth)[None, None, :],
        signed_wave(upward, height)[None, :, None],
        signed_wave(waves_here, total_depth)[:, None, None],
    )
    curl = cross_waves(waves, coeffs)
    all_rows = jnp.arange(total_depth, dtype=jnp.int32)
    wave_rows = reverse_bits(all_rows // depth, levels) + groups * (all_rows % depth)
    height_cos, height_sin = phase_tables(upward, upward, height, 1.0)
    width_cos, width_sin = phase_tables(across, across, breadth, 1.0)
    planar = along_height(curl, height_cos, height_sin)
    planar = along_width(planar, width_cos, width_sin)
    material_slab = lax.all_to_all(material, "gz", split_axis=1, concat_axis=0, tiled=True)
    inverse_cos, inverse_sin = phase_tables(wave_rows, all_rows, total_depth, 1.0)
    forward_cos, forward_sin = phase_tables(all_rows, wave_rows, total_depth, -1.0)
    spatial_piece = along_depth(
        lax.all_to_all(planar, "gz", split_axis=4, concat_axis=3, tiled=True),
        inverse_cos,
        inverse_sin,
    )
    scaled_piece = apply_material(spatial_piece, material_slab, inv_diag, inv_off)
    returned = along_depth(scaled_piece, forward_cos, forward_sin)
    spectral = lax.all_to_all(returned, "gz", split_axis=3, concat_axis=4, tiled=True)
    spectral = along_width(spectral, width_cos, -width_sin)
    spectral = along_height(spectral, height_cos, -height_sin)
    theta = -cross_waves(waves, spectral)
    factor = 1.0 / (breadth * height * total_depth)
    piece = lax.all_gather(coeffs, "ba", axis=2, tiled=True)
    real_part = jnp.einsum("cbzyx,cezyx->be", piece[0], theta[0], precision=highest) + jnp.einsum(
        "cbzyx,cezyx->be", piece[1], theta[1], precision=highest
    )
    imag_part = jnp.einsum("cbzyx,cezyx->be", piece[0], theta[1], precision=highest) - jnp.einsum(
        "cbzyx,cezyx->be", piece[1], theta[0], precision=highest
    )
    block = jnp.stack([real_part, imag_part]) * factor
    gram = lax.psum(block, "gz")
    return (theta, gram)


MESH = pl.DeviceIdType.MESH
single = jnp.float32
half = jnp.bfloat16


def split_table(length, extra):
    numbers = np.arange(length)
    angle = 2.0 * np.pi / length * (numbers[:, None] * numbers[None, :] % length)
    cosine = np.cos(angle) * extra / math.sqrt(length)
    sine = np.sin(angle) * extra / math.sqrt(length)
    inverse = np.block([[cosine, sine], [-sine, cosine]])
    parts = []
    for table in (inverse, inverse.T):
        high = table.astype(np.float32).astype(half)
        low = (table - high.astype(np.float64)).astype(half)
        parts += [high, low]
    return np.stack(parts)


def halves(values):
    high = values.astype(half)
    return high, (values - high.astype(single)).astype(half)


def product(first, second):
    dot = functools.partial(jnp.dot, preferred_element_type=single)
    return dot(first[0], second[0]) + (dot(first[0], second[1]) + dot(first[1], second[0]))


def twiddled(pair, step, span, sign):
    real, imag = pair
    if step == 0:
        return real, imag
    if 2 * step == span:
        return (-imag, real) if sign > 0 else (imag, -real)
    angle = math.pi * step / span
    cosine, sine = math.cos(angle), sign * math.sin(angle)
    return real * cosine - imag * sine, real * sine + imag * cosine


def to_voxels(points):
    points = list(points)
    span = 1
    while span < len(points):
        for base in range(0, len(points), 2 * span):
            for step in range(span):
                a = points[base + step]
                t = twiddled(points[base + step + span], step, span, 1.0)
                points[base + step] = (a[0] + t[0], a[1] + t[1])
                points[base + step + span] = (a[0] - t[0], a[1] - t[1])
        span *= 2
    return points


def to_waves(points):
    points = list(points)
    span = len(points) // 2
    while span >= 1:
        for base in range(0, len(points), 2 * span):
            for step in range(span):
                a, t = points[base + step], points[base + step + span]
                points[base + step] = (a[0] + t[0], a[1] + t[1])
                points[base + step + span] = twiddled(
                    (a[0] - t[0], a[1] - t[1]), step, span, -1.0
                )
        span //= 2
    return points


def operator_kernel(
    groups,
    coeffs_ref,
    material_ref,
    diag_ref,
    off_ref,
    wide_ref,
    tall_ref,
    theta_ref,
    gram_ref,
    other_ref,
    slab_ref,
    tensor_ref,
    high_ref,
    low_ref,
    back_ref,
    field_ref,
    out1_ref,
    in1_ref,
    out2_ref,
    in2_ref,
    sums_ref,
    slab_send,
    slab_recv,
    send1,
    recv1,
    send2,
    recv2,
    other_sem,
    sums_send,
    sums_recv,
):
    _, comps, bands, depth, height, breadth = coeffs_ref.shape
    total = depth * groups
    columns = height // groups
    levels = groups.bit_length() - 1
    me = lax.axis_index("gz")
    mine = lax.axis_index("ba")
    middle = groups // 2

    def offset_of(i):
        away = (i + 1) // 2
        return middle + away - 2 * away * (i % 2)

    def each_peer(body):
        def step(i, carry):
            k = offset_of(i)
            body(k, (me + k) % groups, (me + groups - k) % groups)
            return carry

        lax.fori_loop(0, groups - 1, step, 0)

    barrier = pltpu.get_barrier_semaphore()
    each_peer(
        lambda k, peer, source: pl.semaphore_signal(
            barrier, inc=1, device_id={"gz": peer}, device_id_type=MESH
        )
    )
    pl.semaphore_signal(barrier, inc=1, device_id={"ba": 1 - mine}, device_id_type=MESH)

    across = lax.broadcasted_iota(jnp.int32, (1, breadth), 1)
    upward = lax.broadcasted_iota(jnp.int32, (height, 1), 0)
    wave_x = jnp.where(across < breadth // 2, across, across - breadth).astype(single) / (
        breadth / 2.0
    )
    wave_y = jnp.where(upward < height // 2, upward, upward - height).astype(single) / (
        height / 2.0
    )
    reversed_me = 0
    for position in range(levels):
        reversed_me = reversed_me + (me // (1 << position)) % 2 * (1 << (levels - 1 - position))
    waves_z = []
    for row in range(depth):
        number = reversed_me + groups * row
        signed = number - total * (number // (total // 2))
        waves_z.append(signed.astype(single) / (total / 2.0))

    def cross(parts, row):
        waves = (wave_x, wave_y, waves_z[row])
        return [
            waves[(c + 1) % 3] * parts[(c + 2) % 3] - waves[(c + 2) % 3] * parts[(c + 1) % 3]
            for c in range(3)
        ]

    wide_inv, wide_fwd = (wide_ref[0], wide_ref[1]), (wide_ref[2], wide_ref[3])
    tall_fwd, tall_inv = (tall_ref[0], tall_ref[1]), (tall_ref[2], tall_ref[3])

    def gather_blocks(values):
        top, bottom = values[:height], values[height:]
        return jnp.concatenate(
            [
                jnp.concatenate(
                    [
                        top[:, z * breadth : (z + 1) * breadth],
                        bottom[:, z * breadth : (z + 1) * breadth],
                    ],
                    axis=1,
                )
                for z in range(depth)
            ],
            axis=0,
        )

    def spread_blocks(values):
        return jnp.concatenate(
            [
                jnp.concatenate(
                    [
                        values[z * height : (z + 1) * height, p * breadth : (p + 1) * breadth]
                        for z in range(depth)
                    ],
                    axis=1,
                )
                for p in range(2)
            ],
            axis=0,
        )

    def make_planes(b):
        for p in range(2):
            for z in range(depth):
                curls = cross([coeffs_ref[p, c, b, z] for c in range(3)], z)
                for c in range(3):
                    high, low = halves(curls[c])
                    rows, lanes = pl.ds(p * height, height), pl.ds(z * breadth, breadth)
                    high_ref[c, rows, lanes] = high
                    low_ref[c, rows, lanes] = low

        def one(c, carry):
            tall = product(tall_inv, (high_ref[c], low_ref[c]))
            wide = product(halves(gather_blocks(tall)), wide_inv)
            for p in range(2):
                for z in range(depth):
                    plane = wide[z * height : (z + 1) * height, p * breadth : (p + 1) * breadth]
                    out1_ref[b, :, c, p, z] = plane.reshape(groups, columns, breadth)
            return carry

        lax.fori_loop(0, 3, one, 0)

    def exchange(out, into, send, recv, b, peer, k):
        return pltpu.make_async_remote_copy(
            src_ref=out.at[b, peer],
            dst_ref=into.at[b, me],
            send_sem=send.at[b, k],
            recv_sem=recv.at[b, k],
            device_id={"gz": peer},
            device_id_type=MESH,
        )

    def arrival(out, into, send, recv, b, source, k):
        return pltpu.make_async_remote_copy(
            src_ref=out.at[b, source],
            dst_ref=into.at[b, source],
            send_sem=send.at[b, k],
            recv_sem=recv.at[b, k],
            device_id={"gz": source},
            device_id_type=MESH,
        )

    def start_all(out, into, send, recv, b):
        each_peer(lambda k, peer, source: exchange(out, into, send, recv, b, peer, k).start())
        into[b, me] = out[b, me]

    def finish_all(out, into, send, recv, b):
        each_peer(
            lambda k, peer, source: arrival(out, into, send, recv, b, source, k).wait_recv()
        )

    def drain_all(out, into, send, recv, b):
        each_peer(lambda k, peer, source: exchange(out, into, send, recv, b, peer, k).wait_send())

    def slab_copy(peer, slot, k):
        return pltpu.make_async_remote_copy(
            src_ref=material_ref.at[:, pl.ds(pl.multiple_of(peer * columns, columns), columns), :],
            dst_ref=slab_ref.at[slot],
            send_sem=slab_send.at[k],
            recv_sem=slab_recv.at[k],
            device_id={"gz": peer},
            device_id_type=MESH,
        )

    other_copy = pltpu.make_async_remote_copy(
        src_ref=coeffs_ref,
        dst_ref=other_ref,
        send_sem=other_sem.at[0],
        recv_sem=other_sem.at[1],
        device_id={"ba": 1 - mine},
        device_id_type=MESH,
    )

    make_planes(0)
    pl.semaphore_wait(barrier, groups)
    start_all(out1_ref, in1_ref, send1, recv1, 0)
    each_peer(lambda k, peer, source: slab_copy(peer, me, k).start())
    slab_ref[me] = material_ref[:, pl.ds(pl.multiple_of(me * columns, columns), columns), :]
    other_copy.start()
    for b in range(1, bands):
        make_planes(b)
        start_all(out1_ref, in1_ref, send1, recv1, b)

    each_peer(lambda k, peer, source: slab_copy(source, source, k).wait_recv())
    kinds = diag_ref.shape[0]
    codes = slab_ref[...].reshape(total, columns, breadth)
    for entry in range(6):
        table = diag_ref if entry < 3 else off_ref
        values = jnp.full(codes.shape, table[0, entry % 3], single)
        for kind in range(1, kinds):
            values = jnp.where(codes == kind, table[kind, entry % 3], values)
        tensor_ref[entry] = values

    for b in range(bands):
        finish_all(out1_ref, in1_ref, send1, recv1, b)

        def inverse(c, carry):
            points = [
                (in1_ref[b, r // depth, c, 0, r % depth], in1_ref[b, r // depth, c, 1, r % depth])
                for r in range(total)
            ]
            for z, (real, imag) in enumerate(to_voxels(points)):
                field_ref[c, 0, z] = real
                field_ref[c, 1, z] = imag
            return carry

        lax.fori_loop(0, 3, inverse, 0)

        def scale(z, carry):
            xx, yy, zz, xy, yz, zx = [tensor_ref[entry, z] for entry in range(6)]
            for p in range(2):
                first, second, third = [field_ref[c, p, z] for c in range(3)]
                field_ref[0, p, z] = xx * first + xy * second + zx * third
                field_ref[1, p, z] = xy * first + yy * second + yz * third
                field_ref[2, p, z] = zx * first + yz * second + zz * third
            return carry

        lax.fori_loop(0, total, scale, 0, unroll=4)

        def forward(c, carry):
            points = [(field_ref[c, 0, z], field_ref[c, 1, z]) for z in range(total)]
            for r, (real, imag) in enumerate(to_waves(points)):
                out2_ref[b, r // depth, c, 0, r % depth] = real
                out2_ref[b, r // depth, c, 1, r % depth] = imag
            return carry

        lax.fori_loop(0, 3, forward, 0)
        start_all(out2_ref, in2_ref, send2, recv2, b)

    other_copy.wait()

    def fold(values):
        return jnp.sum(values.reshape(height // 8, 8, breadth), axis=0)

    rows_of = []
    for b in range(bands):
        finish_all(out2_ref, in2_ref, send2, recv2, b)

        def plane_of(c, carry):
            planes = jnp.concatenate(
                [
                    jnp.concatenate(
                        [in2_ref[b, :, c, p, z].reshape(height, breadth) for p in range(2)], axis=1
                    )
                    for z in range(depth)
                ],
                axis=0,
            )
            wide = product(halves(planes), wide_fwd)
            back_ref[c] = product(tall_fwd, halves(spread_blocks(wide)))
            return carry

        lax.fori_loop(0, 3, plane_of, 0)

        for z in range(depth):
            for p in range(2):
                rows, lanes = pl.ds(p * height, height), pl.ds(z * breadth, breadth)
                crossed = cross([back_ref[c, rows, lanes] for c in range(3)], z)
                for c in range(3):
                    theta_ref[p, c, b, z] = -crossed[c]

        def partial(source, a):
            def one(n, sums):
                c, z = n // depth, n % depth
                real, imag = source[0, c, a, z], source[1, c, a, z]
                t_real, t_imag = theta_ref[0, c, b, z], theta_ref[1, c, b, z]
                return (
                    sums[0] + fold(real * t_real + imag * t_imag),
                    sums[1] + fold(real * t_imag - imag * t_real),
                )

            zero = jnp.zeros((8, breadth), single)
            return lax.fori_loop(0, 3 * depth, one, (zero, zero))

        for source in (coeffs_ref, other_ref):
            for a in range(bands):
                for value in partial(source, a):
                    rows_of.append(jnp.sum(value, axis=0, keepdims=True))

    sums_ref[me] = jnp.concatenate(rows_of, axis=0)

    def sums_copy(slot, peer, k):
        return pltpu.make_async_remote_copy(
            src_ref=sums_ref.at[slot],
            dst_ref=sums_ref.at[slot],
            send_sem=sums_send.at[k],
            recv_sem=sums_recv.at[k],
            device_id={"gz": peer},
            device_id_type=MESH,
        )

    each_peer(lambda k, peer, source: sums_copy(me, peer, k).start())
    each_peer(lambda k, peer, source: slab_copy(peer, me, k).wait_send())
    for b in range(bands):
        drain_all(out1_ref, in1_ref, send1, recv1, b)
        drain_all(out2_ref, in2_ref, send2, recv2, b)
    each_peer(lambda k, peer, source: sums_copy(source, source, k).wait_recv())
    gram_ref[...] = jnp.sum(sums_ref[...], axis=0)
    each_peer(lambda k, peer, source: sums_copy(me, peer, k).wait_send())


def on_device_kernel(coeffs, material, inv_diag, inv_off):
    groups = lax.axis_size("gz")
    _, comps, bands, depth, height, breadth = coeffs.shape
    total = depth * groups
    columns = height // groups
    wide = jnp.asarray(split_table(breadth, 1.0 / math.sqrt(total)))
    tall = jnp.asarray(split_table(height, 1.0))
    grams = bands * 4 * bands
    block = (bands, groups, 3, 2, depth, columns, breadth)
    vmem, smem = pl.BlockSpec(memory_space=pltpu.VMEM), pl.BlockSpec(memory_space=pltpu.SMEM)
    dma = pltpu.SemaphoreType.DMA
    theta, sums = pl.pallas_call(
        functools.partial(operator_kernel, groups),
        out_shape=(
            jax.ShapeDtypeStruct(coeffs.shape, single),
            jax.ShapeDtypeStruct((grams, breadth), single),
        ),
        in_specs=[vmem, vmem, smem, smem, vmem, vmem],
        out_specs=(vmem, vmem),
        scratch_shapes=[
            pltpu.VMEM(coeffs.shape, single),
            pltpu.VMEM((groups, depth, columns, breadth), jnp.int32),
            pltpu.VMEM((6, total, columns, breadth), single),
            pltpu.VMEM((3, 2 * height, depth * breadth), half),
            pltpu.VMEM((3, 2 * height, depth * breadth), half),
            pltpu.VMEM((3, 2 * height, depth * breadth), single),
            pltpu.VMEM((3, 2, total, columns, breadth), single),
            pltpu.VMEM(block, single),
            pltpu.VMEM(block, single),
            pltpu.VMEM(block, single),
            pltpu.VMEM(block, single),
            pltpu.VMEM((groups, grams, breadth), single),
            dma((groups,)),
            dma((groups,)),
            dma((bands, groups)),
            dma((bands, groups)),
            dma((bands, groups)),
            dma((bands, groups)),
            dma((2,)),
            dma((groups,)),
            dma((groups,)),
        ],
        compiler_params=pltpu.CompilerParams(
            collective_id=0, has_side_effects=True, vmem_limit_bytes=48 * 1024 * 1024
        ),
        name="maxwell",
    )(coeffs, material, inv_diag, inv_off, wide, tall)
    values = jnp.sum(sums, axis=1) / (breadth * height * total)
    values = values.reshape(bands, 2, bands, 2).transpose(1, 3, 2, 0)
    own, other = values[0], values[1]
    first = lax.axis_index("ba") == 0
    gram = jnp.concatenate([jnp.where(first, own, other), jnp.where(first, other, own)], axis=1)
    return (theta, gram)


def fits(coeffs):
    groups, depth, height, breadth = (
        lax.axis_size("gz"),
        coeffs.shape[3],
        coeffs.shape[4],
        coeffs.shape[5],
    )
    return (
        lax.axis_size("ba") == 2
        and depth == 2
        and height % (8 * groups) == 0
        and height % 128 == 0
        and breadth % 128 == 0
    )


def on_either(coeffs, material, inv_diag, inv_off):
    chosen = on_device_kernel if fits(coeffs) else on_device
    return chosen(coeffs, material, inv_diag, inv_off)


def solution(mesh):
    in_specs = (P(None, None, "ba", "gz", None, None), P("gz", None, None), P(), P())
    out_specs = (P(None, None, "ba", "gz", None, None), P(None, None, "ba"))
    return jax.shard_map(
        on_either, mesh=mesh, in_specs=in_specs, out_specs=out_specs, check_vma=False
    )
```

```python
import functools
import math

import jax
import jax.numpy as jnp
import numpy as np
from jax import lax
from jax.experimental import pallas as pl
from jax.experimental.pallas import tpu as pltpu
from jax.sharding import PartitionSpec as P

highest = lax.Precision.HIGHEST
half_turn = 3.141592653589793


def reverse_bits(values, levels):
    flipped = jnp.zeros_like(values)
    for position in range(levels):
        flipped = flipped + (values >> position & 1) * (1 << levels - 1 - position)
    return flipped


def signed_wave(numbers, length):
    shifted = jnp.where(numbers < length // 2, numbers, numbers - length)
    return shifted.astype(jnp.float32) / (length / 2.0)


def phase_tables(first, second, length, sign):
    product = first[:, None] * second[None, :] % length
    angle = 2.0 * half_turn / length * product.astype(jnp.float32)
    factor = 1.0 / math.sqrt(length)
    return (jnp.cos(angle) * factor, sign * jnp.sin(angle) * factor)


def cross_waves(waves, field):
    first, second, third = waves
    return jnp.stack(
        [
            second * field[:, 2] - third * field[:, 1],
            third * field[:, 0] - first * field[:, 2],
            first * field[:, 1] - second * field[:, 0],
        ],
        axis=1,
    )


def along_width(field, cosine, sine):
    breadth = field.shape[-1]
    rows = field.reshape(2, -1, breadth)
    joined = jnp.concatenate([cosine, sine], axis=1)
    real_prod = jnp.dot(rows[0], joined, precision=highest)
    imag_prod = jnp.dot(rows[1], joined, precision=highest)
    real_out = real_prod[:, :breadth] - imag_prod[:, breadth:]
    imag_out = real_prod[:, breadth:] + imag_prod[:, :breadth]
    return jnp.stack([real_out, imag_out]).reshape(field.shape)


def along_height(field, cosine, sine):
    tables = jnp.stack([cosine, sine])
    product = jnp.einsum("pcbzyx,tyk->tpcbzkx", field, tables, precision=highest)
    return jnp.stack([product[0, 0] - product[1, 1], product[1, 0] + product[0, 1]])


def along_depth(field, cosine, sine):
    tables = jnp.stack([cosine, sine])
    product = jnp.einsum("pcbzyx,tzk->tpcbkyx", field, tables, precision=highest)
    return jnp.stack([product[0, 0] - product[1, 1], product[1, 0] + product[0, 1]])


def apply_material(field, material, inv_diag, inv_off):
    materials = inv_diag.shape[0]
    onehot = (material[None] == jnp.arange(materials, dtype=jnp.int32)[:, None, None, None]).astype(
        jnp.float32
    )
    table = jnp.concatenate([inv_diag, inv_off], axis=1)
    tensor = jnp.einsum("mk,mzyx->kzyx", table, onehot, precision=highest)
    first = field[:, 0]
    second = field[:, 1]
    third = field[:, 2]
    return jnp.stack(
        [
            tensor[0] * first + tensor[3] * second + tensor[5] * third,
            tensor[3] * first + tensor[1] * second + tensor[4] * third,
            tensor[5] * first + tensor[4] * second + tensor[2] * third,
        ],
        axis=1,
    )


def on_device(coeffs, material, inv_diag, inv_off):
    groups = lax.axis_size("gz")
    levels = groups.bit_length() - 1
    depth = coeffs.shape[3]
    height = coeffs.shape[4]
    breadth = coeffs.shape[5]
    total_depth = depth * groups
    device = lax.axis_index("gz")
    local_rows = jnp.arange(depth, dtype=jnp.int32)
    waves_here = reverse_bits(device, levels) + groups * local_rows
    across = jnp.arange(breadth, dtype=jnp.int32)
    upward = jnp.arange(height, dtype=jnp.int32)
    waves = (
        signed_wave(across, breadth)[None, None, :],
        signed_wave(upward, height)[None, :, None],
        signed_wave(waves_here, total_depth)[:, None, None],
    )
    curl = cross_waves(waves, coeffs)
    all_rows = jnp.arange(total_depth, dtype=jnp.int32)
    wave_rows = reverse_bits(all_rows // depth, levels) + groups * (all_rows % depth)
    height_cos, height_sin = phase_tables(upward, upward, height, 1.0)
    width_cos, width_sin = phase_tables(across, across, breadth, 1.0)
    planar = along_height(curl, height_cos, height_sin)
    planar = along_width(planar, width_cos, width_sin)
    material_slab = lax.all_to_all(material, "gz", split_axis=1, concat_axis=0, tiled=True)
    inverse_cos, inverse_sin = phase_tables(wave_rows, all_rows, total_depth, 1.0)
    forward_cos, forward_sin = phase_tables(all_rows, wave_rows, total_depth, -1.0)
    spatial_piece = along_depth(
        lax.all_to_all(planar, "gz", split_axis=4, concat_axis=3, tiled=True),
        inverse_cos,
        inverse_sin,
    )
    scaled_piece = apply_material(spatial_piece, material_slab, inv_diag, inv_off)
    returned = along_depth(scaled_piece, forward_cos, forward_sin)
    spectral = lax.all_to_all(returned, "gz", split_axis=3, concat_axis=4, tiled=True)
    spectral = along_width(spectral, width_cos, -width_sin)
    spectral = along_height(spectral, height_cos, -height_sin)
    theta = -cross_waves(waves, spectral)
    factor = 1.0 / (breadth * height * total_depth)
    piece = lax.all_gather(coeffs, "ba", axis=2, tiled=True)
    real_part = jnp.einsum("cbzyx,cezyx->be", piece[0], theta[0], precision=highest) + jnp.einsum(
        "cbzyx,cezyx->be", piece[1], theta[1], precision=highest
    )
    imag_part = jnp.einsum("cbzyx,cezyx->be", piece[0], theta[1], precision=highest) - jnp.einsum(
        "cbzyx,cezyx->be", piece[1], theta[0], precision=highest
    )
    block = jnp.stack([real_part, imag_part]) * factor
    gram = lax.psum(block, "gz")
    return (theta, gram)


MESH = pl.DeviceIdType.MESH
single = jnp.float32
half = jnp.bfloat16


def split_table(length, extra):
    numbers = np.arange(length)
    angle = 2.0 * np.pi / length * (numbers[:, None] * numbers[None, :] % length)
    cosine = np.cos(angle) * extra / math.sqrt(length)
    sine = np.sin(angle) * extra / math.sqrt(length)
    inverse = np.block([[cosine, sine], [-sine, cosine]])
    parts = []
    for table in (inverse, inverse.T):
        high = table.astype(np.float32).astype(half)
        low = (table - high.astype(np.float64)).astype(half)
        parts += [high, low]
    return np.stack(parts)


def halves(values):
    high = values.astype(half)
    return high, (values - high.astype(single)).astype(half)


def product(first, second):
    dot = functools.partial(jnp.dot, preferred_element_type=single)
    return dot(first[0], second[0]) + (dot(first[0], second[1]) + dot(first[1], second[0]))


def twiddled(pair, step, span, sign):
    real, imag = pair
    if step == 0:
        return real, imag
    if 2 * step == span:
        return (-imag, real) if sign > 0 else (imag, -real)
    angle = math.pi * step / span
    cosine, sine = math.cos(angle), sign * math.sin(angle)
    return real * cosine - imag * sine, real * sine + imag * cosine


def to_voxels(points):
    points = list(points)
    span = 1
    while span < len(points):
        for base in range(0, len(points), 2 * span):
            for step in range(span):
                a = points[base + step]
                t = twiddled(points[base + step + span], step, span, 1.0)
                points[base + step] = (a[0] + t[0], a[1] + t[1])
                points[base + step + span] = (a[0] - t[0], a[1] - t[1])
        span *= 2
    return points


def to_waves(points):
    points = list(points)
    span = len(points) // 2
    while span >= 1:
        for base in range(0, len(points), 2 * span):
            for step in range(span):
                a, t = points[base + step], points[base + step + span]
                points[base + step] = (a[0] + t[0], a[1] + t[1])
                points[base + step + span] = twiddled(
                    (a[0] - t[0], a[1] - t[1]), step, span, -1.0
                )
        span //= 2
    return points


def operator_kernel(
    groups,
    coeffs_hbm,
    material_hbm,
    diag_hbm,
    off_hbm,
    table_hbm,
    theta_ref,
    gram_ref,
    coeffs_ref,
    material_ref,
    table_ref,
    diag_ref,
    off_ref,
    slab_ref,
    tensor_ref,
    high_ref,
    low_ref,
    back_ref,
    field_ref,
    scaled_ref,
    other_ref,
    out1_ref,
    in1_ref,
    out2_ref,
    in2_ref,
    sums_ref,
    load_sem,
    slab_send,
    slab_recv,
    half_sem,
    send1,
    recv1,
    send2,
    recv2,
    other_send,
    other_recv,
    sums_send,
    sums_recv,
):
    _, comps, bands, depth, height, breadth = coeffs_ref.shape
    total = depth * groups
    columns = height // groups
    levels = groups.bit_length() - 1
    me = lax.axis_index("gz")
    mine = lax.axis_index("ba")
    middle = groups // 2

    def offset_of(i):
        away = (i + 1) // 2
        return middle + away - 2 * away * (i % 2)

    def each_peer(body):
        def step(i, carry):
            k = offset_of(i)
            body(k, (me + k) % groups, (me + groups - k) % groups)
            return carry

        lax.fori_loop(0, groups - 1, step, 0)

    barrier = pltpu.get_barrier_semaphore()
    each_peer(
        lambda k, peer, source: pl.semaphore_signal(
            barrier, inc=1, device_id={"gz": peer}, device_id_type=MESH
        )
    )
    pl.semaphore_signal(barrier, inc=1, device_id={"ba": 1 - mine}, device_id_type=MESH)

    loads = [
        pltpu.make_async_copy(coeffs_hbm, coeffs_ref, load_sem.at[0]),
        pltpu.make_async_copy(table_hbm, table_ref, load_sem.at[1]),
        pltpu.make_async_copy(material_hbm, material_ref, load_sem.at[2]),
        pltpu.make_async_copy(diag_hbm, diag_ref, load_sem.at[3]),
        pltpu.make_async_copy(off_hbm, off_ref, load_sem.at[4]),
    ]
    for load in loads:
        load.start()

    across = lax.broadcasted_iota(jnp.int32, (1, breadth), 1)
    upward = lax.broadcasted_iota(jnp.int32, (height, 1), 0)
    wave_x = jnp.where(across < breadth // 2, across, across - breadth).astype(single) / (
        breadth / 2.0
    )
    wave_y = jnp.where(upward < height // 2, upward, upward - height).astype(single) / (
        height / 2.0
    )
    reversed_me = 0
    for position in range(levels):
        reversed_me = reversed_me + (me // (1 << position)) % 2 * (1 << (levels - 1 - position))
    waves_z = []
    for row in range(depth):
        number = reversed_me + groups * row
        signed = number - total * (number // (total // 2))
        waves_z.append(signed.astype(single) / (total / 2.0))

    def cross(parts, row):
        waves = (wave_x, wave_y, waves_z[row])
        return [
            waves[(c + 1) % 3] * parts[(c + 2) % 3] - waves[(c + 2) % 3] * parts[(c + 1) % 3]
            for c in range(3)
        ]

    def plain_table():
        return table_ref[0], table_ref[1]

    def turned_table():
        return table_ref[2], table_ref[3]

    def gather_blocks(values):
        top, bottom = values[:height], values[height:]
        return jnp.concatenate(
            [
                jnp.concatenate(
                    [
                        top[:, z * breadth : (z + 1) * breadth],
                        bottom[:, z * breadth : (z + 1) * breadth],
                    ],
                    axis=1,
                )
                for z in range(depth)
            ],
            axis=0,
        )

    def spread_blocks(values):
        return jnp.concatenate(
            [
                jnp.concatenate(
                    [
                        values[z * height : (z + 1) * height, p * breadth : (p + 1) * breadth]
                        for z in range(depth)
                    ],
                    axis=1,
                )
                for p in range(2)
            ],
            axis=0,
        )

    def make_planes(b):
        for p in range(2):
            for z in range(depth):
                curls = cross([coeffs_ref[p, c, b, z] for c in range(3)], z)
                for c in range(3):
                    high, low = halves(curls[c])
                    rows, lanes = pl.ds(p * height, height), pl.ds(z * breadth, breadth)
                    high_ref[c, rows, lanes] = high
                    low_ref[c, rows, lanes] = low

        def one(c, carry):
            tall = product(turned_table(), (high_ref[c], low_ref[c]))
            wide = product(halves(gather_blocks(tall)), plain_table())
            for p in range(2):
                for z in range(depth):
                    plane = wide[z * height : (z + 1) * height, p * breadth : (p + 1) * breadth]
                    out1_ref[b, :, c, p, z] = plane.reshape(groups, columns, breadth)
            return carry

        lax.fori_loop(0, 3, one, 0)

    def exchange(out, into, send, recv, b, peer, k):
        return pltpu.make_async_remote_copy(
            src_ref=out.at[b, peer],
            dst_ref=into.at[b, me],
            send_sem=send.at[b, k],
            recv_sem=recv.at[b, k],
            device_id={"gz": peer},
            device_id_type=MESH,
        )

    def arrival(out, into, send, recv, b, source, k):
        return pltpu.make_async_remote_copy(
            src_ref=out.at[b, source],
            dst_ref=into.at[b, source],
            send_sem=send.at[b, k],
            recv_sem=recv.at[b, k],
            device_id={"gz": source},
            device_id_type=MESH,
        )

    def start_all(out, into, send, recv, b):
        each_peer(lambda k, peer, source: exchange(out, into, send, recv, b, peer, k).start())
        into[b, me] = out[b, me]

    def finish_all(out, into, send, recv, b):
        each_peer(
            lambda k, peer, source: arrival(out, into, send, recv, b, source, k).wait_recv()
        )

    def drain_all(out, into, send, recv, b):
        each_peer(lambda k, peer, source: exchange(out, into, send, recv, b, peer, k).wait_send())

    def columns_of(peer):
        return pl.ds(pl.multiple_of(peer * columns, columns), columns)

    def slab_copy(peer, slot, k):
        return pltpu.make_async_remote_copy(
            src_ref=material_ref.at[mine, columns_of(peer), :],
            dst_ref=slab_ref.at[mine, slot],
            send_sem=slab_send.at[k],
            recv_sem=slab_recv.at[k],
            device_id={"gz": peer},
            device_id_type=MESH,
        )

    def half_copy(row):
        return pltpu.make_async_remote_copy(
            src_ref=slab_ref.at[row],
            dst_ref=slab_ref.at[row],
            send_sem=half_sem.at[0],
            recv_sem=half_sem.at[1],
            device_id={"ba": 1 - mine},
            device_id_type=MESH,
        )

    def other_copy(b):
        return pltpu.make_async_remote_copy(
            src_ref=field_ref.at[b],
            dst_ref=other_ref.at[b],
            send_sem=other_send.at[b],
            recv_sem=other_recv.at[b],
            device_id={"ba": 1 - mine},
            device_id_type=MESH,
        )

    loads[0].wait()
    loads[1].wait()
    make_planes(0)
    for load in loads[2:]:
        load.wait()
    pl.semaphore_wait(barrier, groups)
    start_all(out1_ref, in1_ref, send1, recv1, 0)
    each_peer(lambda k, peer, source: slab_copy(peer, me, k).start())
    slab_ref[mine, me] = material_ref[mine, columns_of(me), :]
    for b in range(1, bands):
        make_planes(b)
        start_all(out1_ref, in1_ref, send1, recv1, b)

    each_peer(lambda k, peer, source: slab_copy(source, source, k).wait_recv())
    half_copy(mine).start()
    half_copy(1 - mine).wait_recv()
    kinds = diag_ref.shape[0]
    for row in range(depth):
        codes = slab_ref[row]
        for entry in range(6):
            table = diag_ref if entry < 3 else off_ref
            values = jnp.full(codes.shape, table[0, entry % 3], single)
            for kind in range(1, kinds):
                values = jnp.where(codes == kind, table[kind, entry % 3], values)
            tensor_ref[entry, :, row] = values

    for b in range(bands):
        finish_all(out1_ref, in1_ref, send1, recv1, b)

        def inverse(c, carry):
            points = [
                (in1_ref[b, r // depth, c, 0, r % depth], in1_ref[b, r // depth, c, 1, r % depth])
                for r in range(total)
            ]
            for z, (real, imag) in enumerate(to_voxels(points)):
                field_ref[b, c, 0, z] = real
                field_ref[b, c, 1, z] = imag
            return carry

        lax.fori_loop(0, 3, inverse, 0)
        other_copy(b).start()

        def scale(z, carry):
            xx, yy, zz, xy, yz, zx = [
                tensor_ref[entry, z // depth, z % depth] for entry in range(6)
            ]
            for p in range(2):
                first, second, third = [field_ref[b, c, p, z] for c in range(3)]
                scaled_ref[b, 0, p, z] = xx * first + xy * second + zx * third
                scaled_ref[b, 1, p, z] = xy * first + yy * second + yz * third
                scaled_ref[b, 2, p, z] = zx * first + yz * second + zz * third
            return carry

        lax.fori_loop(0, total, scale, 0, unroll=4)

        def forward(c, carry):
            points = [(scaled_ref[b, c, 0, z], scaled_ref[b, c, 1, z]) for z in range(total)]
            for r, (real, imag) in enumerate(to_waves(points)):
                out2_ref[b, r // depth, c, 0, r % depth] = real
                out2_ref[b, r // depth, c, 1, r % depth] = imag
            return carry

        lax.fori_loop(0, 3, forward, 0)
        start_all(out2_ref, in2_ref, send2, recv2, b)

    def sums_copy(slot, peer, k):
        return pltpu.make_async_remote_copy(
            src_ref=sums_ref.at[slot],
            dst_ref=sums_ref.at[slot],
            send_sem=sums_send.at[k],
            recv_sem=sums_recv.at[k],
            device_id={"gz": peer},
            device_id_type=MESH,
        )

    def make_sums():
        def add(z, sums):
            sums = list(sums)
            for c in range(3):
                ours = [(scaled_ref[b, c, 0, z], scaled_ref[b, c, 1, z]) for b in range(bands)]
                fields = [
                    (source[a, c, 0, z], source[a, c, 1, z])
                    for source in (field_ref, other_ref)
                    for a in range(bands)
                ]
                n = 0
                for t_real, t_imag in ours:
                    for real, imag in fields:
                        sums[n] = sums[n] + (real * t_real + imag * t_imag)
                        sums[n + 1] = sums[n + 1] + (real * t_imag - imag * t_real)
                        n += 2
            return tuple(sums)

        zero = jnp.zeros((columns, breadth), single)
        sums = lax.fori_loop(0, total, add, (zero,) * (4 * bands * bands))
        sums_ref[me] = jnp.concatenate([jnp.sum(v, axis=0, keepdims=True) for v in sums], axis=0)

    half_copy(mine).wait_send()
    each_peer(lambda k, peer, source: slab_copy(peer, me, k).wait_send())
    for b in range(bands):
        drain_all(out1_ref, in1_ref, send1, recv1, b)

    for b in range(bands):
        if b == bands - 1:
            for a in range(bands):
                other_copy(a).wait_send()
                other_copy(a).wait_recv()
            make_sums()
            each_peer(lambda k, peer, source: sums_copy(me, peer, k).start())
            for a in range(b):
                drain_all(out2_ref, in2_ref, send2, recv2, a)
        finish_all(out2_ref, in2_ref, send2, recv2, b)

        def plane_of(c, carry):
            planes = jnp.concatenate(
                [
                    jnp.concatenate(
                        [in2_ref[b, :, c, p, z].reshape(height, breadth) for p in range(2)], axis=1
                    )
                    for z in range(depth)
                ],
                axis=0,
            )
            wide = product(halves(planes), turned_table())
            back_ref[c] = product(plain_table(), halves(spread_blocks(wide)))
            return carry

        lax.fori_loop(0, 3, plane_of, 0)

        for z in range(depth):
            for p in range(2):
                rows, lanes = pl.ds(p * height, height), pl.ds(z * breadth, breadth)
                crossed = cross([back_ref[c, rows, lanes] for c in range(3)], z)
                for c in range(3):
                    theta_ref[p, c, b, z] = -crossed[c]

    drain_all(out2_ref, in2_ref, send2, recv2, bands - 1)
    each_peer(lambda k, peer, source: sums_copy(source, source, k).wait_recv())
    gram_ref[...] = jnp.sum(sums_ref[...], axis=0)
    each_peer(lambda k, peer, source: sums_copy(me, peer, k).wait_send())


def on_device_kernel(coeffs, material, inv_diag, inv_off):
    groups = lax.axis_size("gz")
    _, comps, bands, depth, height, breadth = coeffs.shape
    total = depth * groups
    columns = height // groups
    table = jnp.asarray(split_table(breadth, total**-0.25))
    grams = bands * 4 * bands
    voxels = (bands, 3, 2, total, columns, breadth)
    block = (bands, groups, 3, 2, depth, columns, breadth)
    vmem = pl.BlockSpec(memory_space=pltpu.VMEM)
    hbm = pl.BlockSpec(memory_space=pltpu.HBM)
    dma = pltpu.SemaphoreType.DMA
    theta, sums = pl.pallas_call(
        functools.partial(operator_kernel, groups),
        out_shape=(
            jax.ShapeDtypeStruct(coeffs.shape, single),
            jax.ShapeDtypeStruct((grams, breadth), single),
        ),
        in_specs=[hbm, hbm, hbm, hbm, hbm],
        out_specs=(vmem, vmem),
        scratch_shapes=[
            pltpu.VMEM(coeffs.shape, single),
            pltpu.VMEM(material.shape, jnp.int32),
            pltpu.VMEM(table.shape, half),
            pltpu.SMEM(inv_diag.shape, single),
            pltpu.SMEM(inv_off.shape, single),
            pltpu.VMEM((depth, groups, columns, breadth), jnp.int32),
            pltpu.VMEM((6, groups, depth, columns, breadth), single),
            pltpu.VMEM((3, 2 * height, depth * breadth), half),
            pltpu.VMEM((3, 2 * height, depth * breadth), half),
            pltpu.VMEM((3, 2 * height, depth * breadth), single),
            pltpu.VMEM(voxels, single),
            pltpu.VMEM(voxels, single),
            pltpu.VMEM(voxels, single),
            pltpu.VMEM(block, single),
            pltpu.VMEM(block, single),
            pltpu.VMEM(block, single),
            pltpu.VMEM(block, single),
            pltpu.VMEM((groups, grams, breadth), single),
            dma((5,)),
            dma((groups,)),
            dma((groups,)),
            dma((2,)),
            dma((bands, groups)),
            dma((bands, groups)),
            dma((bands, groups)),
            dma((bands, groups)),
            dma((bands,)),
            dma((bands,)),
            dma((groups,)),
            dma((groups,)),
        ],
        compiler_params=pltpu.CompilerParams(
            collective_id=0, has_side_effects=True, vmem_limit_bytes=48 * 1024 * 1024
        ),
        name="maxwell",
    )(coeffs, material, inv_diag, inv_off, table)
    values = jnp.sum(sums, axis=1) / (breadth * height * total)
    values = values.reshape(bands, 2, bands, 2).transpose(1, 3, 2, 0)
    own, other = values[0], values[1]
    first = lax.axis_index("ba") == 0
    gram = jnp.concatenate([jnp.where(first, own, other), jnp.where(first, other, own)], axis=1)
    return (theta, gram)


def fits(coeffs):
    groups, depth, height, breadth = (
        lax.axis_size("gz"),
        coeffs.shape[3],
        coeffs.shape[4],
        coeffs.shape[5],
    )
    return (
        lax.axis_size("ba") == 2
        and depth == 2
        and height % (8 * groups) == 0
        and height == breadth
        and breadth % 128 == 0
    )


def on_either(coeffs, material, inv_diag, inv_off):
    chosen = on_device_kernel if fits(coeffs) else on_device
    return chosen(coeffs, material, inv_diag, inv_off)


def solution(mesh):
    in_specs = (P(None, None, "ba", "gz", None, None), P("gz", None, None), P(), P())
    out_specs = (P(None, None, "ba", "gz", None, None), P(None, None, "ba"))
    return jax.shard_map(
        on_either, mesh=mesh, in_specs=in_specs, out_specs=out_specs, check_vma=False
    )
```
